32 devices in a mesh: dp: 4 (over z), mp: 4 (over y, x), mc: 2 (over core).
Axes of the slice: x: 2, y: 2, z: 4, core: 2. Of those that a mesh axis runs over, the one named last changes fastest.
Arguments:
- features: bfloat16 [1576, 768], P('dp'), may hold values from -6 to 6
- out_cotangent: bfloat16 [2, 1576, 768], P('mc', 'dp'), may hold values from -6 to 6
- mean_up: float32 [768, 3072], P('dp', 'mp'), may hold values from -0.21875 to 0.21875
- precision_up: float32 [768, 3072], P('dp', 'mp'), may hold values from 4 to 64
- noise_up: float32 [2, 768, 3072], P('mc', 'dp', 'mp'), may hold values from -6 to 6
- mean_down: float32 [768, 3072], P('dp', 'mp'), may hold values from -0.109375 to 0.109375
- precision_down: float32 [768, 3072], P('dp', 'mp'), may hold values from 4 to 64
- noise_down: float32 [2, 768, 3072], P('mc', 'dp', 'mp'), may hold values from -6 to 6
Outputs:
- mean_new_up: float32 [768, 3072], P('dp', 'mp')
- precision_new_up: float32 [768, 3072], P('dp', 'mp')
- mean_new_down: float32 [768, 3072], P('dp', 'mp')
- precision_new_down: float32 [768, 3072], P('dp', 'mp')
- input_grad: bfloat16 [2, 1576, 768], P('mc', 'dp', 'mp')
The draws below stay inside these ranges and needn't reach their ends.
All inputs are finite; a program needn't handle non-finite values.
Results may differ from the reference program's by a relative error of at most 0.0015.
The reference program's roundings to bfloat16 on the way (of `hidden` and `preact_grad`) count: a program that leaves them out, or rounds other values in their place, can miss the bound.
Values may be sent and summed in bfloat16 or wider, within the bound.
A program may use at most 64 MiB of HBM per device.

```python
import math
import jax
import jax.numpy as jnp
from jax import lax

D = 768
FF = 3072
PATCHES = 197
MC = 2
IMAGES = 8
TOKENS = 1576


def raised(result, key, source, target, blocks, factor):
    def block_of(axis_at):
        return (jnp.arange(result.shape[axis_at]) // (result.shape[axis_at] // blocks)).reshape((-1,) + (1,) * (result.ndim - 1 - axis_at))

    one_side = jax.random.permutation(key, blocks)[block_of(target)]
    other_side = (block_of(target) + blocks // 2) % blocks
    return jnp.where((block_of(source) == one_side) | (block_of(source) == other_side), factor * result, result)


def block_scale(rng, extent, cuts, low, largest):
    level, own = 1.0, jax.random.fold_in(rng, 6)
    for position, shards_of in cuts:
        steps = jnp.exp(jax.random.uniform(jax.random.fold_in(own, position), (shards_of,), jnp.float32, low / len(cuts), largest / len(cuts)))
        level = level * jnp.repeat(steps, extent[position] // shards_of).reshape([-1 if axis == position else 1 for axis in range(len(extent))])
    return level


def scatter_about(stream_key, dims, width, limit, split=(), held_as=jnp.bfloat16):
    drawn = width * jax.random.normal(stream_key, dims, jnp.float32)
    if split:
        drawn = drawn * block_scale(stream_key, dims, split, -0.22, 0.18)
    return jnp.clip(drawn, -limit, limit).astype(held_as)


def bell_draw_with(own_key, extent, scale, bound, split, heavy, dtype=jnp.bfloat16):
    values = scale * jax.random.normal(own_key, extent, jnp.float32)
    if split:
        values = values * block_scale(own_key, extent, split, -0.22, 0.18)
    return jnp.clip(raised(values, jax.random.fold_in(own_key, 3), *heavy), -bound, bound).astype(dtype)


def setup_inputs(seed: int = 0) -> dict:
    key_list = jax.random.split(jax.random.key(seed), 9)
    return {
        "features": bell_draw_with(key_list[0], (TOKENS, D), 1.0, 6.0, ((0, 4),), (0, 1, 4, 2.0)),
        "out_cotangent": bell_draw_with(key_list[1], (MC, TOKENS, D), 1.0, 6.0, ((0, 2), (1, 4)), (1, 2, 4, 2.0)),
        "mean_up": scatter_about(key_list[2], (D, FF), D ** -0.5, 0.21875, ((0, 4), (1, 4)), jnp.float32),
        "precision_up": jnp.clip(jnp.exp(math.log(64.0) - 2.7725887 * jax.random.uniform(key_list[3], (D, FF), jnp.float32) ** block_scale(key_list[3], (D, FF), ((0, 4), (1, 4)), -0.2, 0.2)), 4.0, 64.0),
        "noise_up": scatter_about(key_list[4], (MC, D, FF), 1.0, 6.0, ((0, 2), (1, 4), (2, 4)), jnp.float32),
        "mean_down": scatter_about(key_list[5], (D, FF), FF ** -0.5, 0.109375, ((0, 4), (1, 4)), jnp.float32),
        "precision_down": jnp.clip(jnp.exp(math.log(64.0) - 2.7725887 * jax.random.uniform(key_list[6], (D, FF), jnp.float32) ** block_scale(key_list[6], (D, FF), ((0, 4), (1, 4)), -0.2, 0.2)), 4.0, 64.0),
        "noise_down": scatter_about(key_list[7], (MC, D, FF), 1.0, 6.0, ((0, 2), (1, 4), (2, 4)), jnp.float32),
    }


reciprocal_root = 0.7071067811865476
normal_peak = 0.3989422804014327
tempering = 100.0
damping = 4.0
average_rate = 0.25
step_rate = 0.05
clip_level = 0.01

def gelu_parts(preact):
    cumulative = 0.5 * (1.0 + lax.erf(preact * reciprocal_root))
    density = normal_peak * jnp.exp(-0.5 * preact * preact)
    return (preact * cumulative, cumulative + preact * density)

def sample_weights(center, precision, noise_draw):
    spread = 1.0 / jnp.sqrt(tempering * (precision + damping))
    return (center + spread * noise_draw).astype(jnp.bfloat16)

def contract_rows(left, right):
    return lax.dot_general(left, right, (((0,), (0,)), ((), ())), preferred_element_type=jnp.float32)

def contract_cols(left, right):
    return lax.dot_general(left, right, (((1,), (1,)), ((), ())), preferred_element_type=jnp.float32)

def reference(features, out_cotangent, mean_up, precision_up, noise_up, mean_down, precision_down, noise_down):
    images = features.shape[0] // PATCHES
    pictures = features.reshape(images, PATCHES, D)
    empty_sum = jnp.zeros((D, FF), jnp.float32)
    running = (empty_sum, empty_sum, empty_sum, empty_sum)
    gradients = []
    for sample_index in range(MC):
        w_up = sample_weights(mean_up, precision_up, noise_up[sample_index])
        w_down = sample_weights(mean_down, precision_down, noise_down[sample_index])
        cotangent = out_cotangent[sample_index].reshape(images, PATCHES, D)

        def per_image(totals, image_pair):
            image_rows, cotangent_rows = image_pair
            preact = jnp.dot(image_rows, w_up, preferred_element_type=jnp.float32)
            gelu_value, gelu_slope = gelu_parts(preact)
            hidden = gelu_value.astype(jnp.bfloat16)
            hidden_grad = jnp.dot(cotangent_rows, w_down, preferred_element_type=jnp.float32)
            preact_grad = (hidden_grad * gelu_slope).astype(jnp.bfloat16)
            input_rows = contract_cols(preact_grad, w_up).astype(jnp.bfloat16)
            grad_up = contract_rows(image_rows, preact_grad)
            grad_down = contract_rows(cotangent_rows, hidden)
            updated = (totals[0] + grad_up, totals[1] + grad_up * grad_up, totals[2] + grad_down, totals[3] + grad_down * grad_down)
            return (updated, input_rows)
        running, input_rows = lax.scan(per_image, running, (pictures, cotangent))
        gradients.append(input_rows.reshape(images * PATCHES, D))
    input_grad = jnp.stack(gradients)
    grad_up = running[0] / MC
    square_up = running[1] / (MC * IMAGES)
    grad_down = running[2] / MC
    square_down = running[3] / (MC * IMAGES)
    precision_new_up = (1.0 - average_rate) * precision_up + average_rate * square_up
    precision_new_down = (1.0 - average_rate) * precision_down + average_rate * square_down
    raw_up = grad_up / (precision_new_up + damping)
    raw_down = grad_down / (precision_new_down + damping)
    global_sum = jnp.sum(raw_up * raw_up) + jnp.sum(raw_down * raw_down)
    root_mean = jnp.sqrt(global_sum / (2 * D * FF))
    factor = 1.0 / jnp.maximum(clip_level, root_mean)
    mean_new_up = mean_up - step_rate * factor * raw_up
    mean_new_down = mean_down - step_rate * factor * raw_down
    return (mean_new_up, precision_new_up, mean_new_down, precision_new_down, input_grad)
```

```python
import functools

import jax
import jax.numpy as jnp
from jax import lax
from jax.experimental import pallas as pl
from jax.experimental.pallas import tpu as pltpu
from jax.sharding import PartitionSpec as P

D = 768
FF = 3072
PATCHES = 197


reciprocal_root = 0.7071067811865476
normal_peak = 0.3989422804014327
tempering = 100.0
damping = 4.0
average_rate = 0.25
step_rate = 0.05
clip_level = 0.01


def gelu_parts(preact):
    cumulative = 0.5 * (1.0 + lax.erf(preact * reciprocal_root))
    density = normal_peak * jnp.exp(-0.5 * preact * preact)
    return (preact * cumulative, cumulative + preact * density)


def sample_weights(center, precision, noise_draw):
    spread = 1.0 / jnp.sqrt(tempering * (precision + damping))
    return (center + spread * noise_draw).astype(jnp.bfloat16)


def contract_rows(left, right):
    return lax.dot_general(
        left, right, (((0,), (0,)), ((), ())), preferred_element_type=jnp.float32
    )


def contract_cols(left, right):
    return lax.dot_general(
        left, right, (((1,), (1,)), ((), ())), preferred_element_type=jnp.float32
    )


def image_sums(rows, grads):
    total = square = None
    for offset in range(0, rows.shape[0], PATCHES):
        grad = contract_rows(rows[offset : offset + PATCHES], grads[offset : offset + PATCHES])
        total = grad if total is None else total + grad
        square = grad * grad if square is None else square + grad * grad
    return total, square


def rows_for(value, core):
    blocks = value.reshape(lax.axis_size("dp"), 2, -1, value.shape[1])
    return lax.dynamic_index_in_dim(blocks, core, 1, keepdims=False)


def exchange_steps(axis):
    ranks = lax.axis_size(axis)
    me = lax.axis_index(axis)
    power = ranks & (ranks - 1) == 0
    for step in range(ranks - 1, 0, -1):
        if power:
            yield me ^ step, [(rank, rank ^ step) for rank in range(ranks)]
        else:
            yield lax.rem(me + step, ranks), [(rank, (rank + step) % ranks) for rank in range(ranks)]


def reduce_images(total, square):
    core = lax.axis_index("mc")
    me = lax.axis_index("dp")
    theirs = jnp.stack([rows_for(total, 1 - core), rows_for(square, 1 - core)], 1)
    ours = jnp.stack([rows_for(total, core), rows_for(square, core)], 1)
    both = ours + lax.ppermute(theirs, "mc", [(0, 1), (1, 0)])
    result = lax.dynamic_index_in_dim(both, me, 0, keepdims=False)
    largest = jnp.maximum(jnp.max(jnp.abs(both), axis=(0, 2), keepdims=True)[0], 1e-30)
    coded = (both * (16384.0 / largest)).astype(jnp.float16)
    scale = largest / 16384.0
    for target, perm in exchange_steps("dp"):
        block = lax.dynamic_index_in_dim(coded, target, 0, keepdims=False)
        arrived = lax.ppermute(block, "dp", perm).astype(jnp.float32)
        result = result + arrived * lax.ppermute(scale, "dp", perm)
    return result


def scatter_sum(value):
    width = value.shape[1] // lax.axis_size("mp")
    result = lax.dynamic_slice_in_dim(value, lax.axis_index("mp") * width, width, 1)
    for target, perm in exchange_steps("mp"):
        block = lax.dynamic_slice_in_dim(value, target * width, width, 1)
        result = result + lax.ppermute(block, "mp", perm)
    return result


def finish_kernel(
    axes, images_all, sums_up, sums_down, precision_up, precision_down, out, total, parts, got, *sems
):
    swap_send, swap_recv, part_send, part_recv = sems
    place = {name: lax.axis_index(name) for name, _ in axes}
    core = place["mc"]
    barrier = pltpu.get_barrier_semaphore()
    count = 0
    for name, size in axes:
        for shift in range(1, size):
            pl.semaphore_signal(
                barrier,
                inc=1,
                device_id={name: lax.rem(place[name] + shift, size)},
                device_id_type=pl.DeviceIdType.MESH,
            )
            count += 1
    local = jnp.zeros((1, out.shape[-1]), jnp.float32)
    for at, (sums, precision) in enumerate(((sums_up, precision_up), (sums_down, precision_down))):
        grad = sums[0] / 2
        square = sums[1] / (2 * images_all)
        fresh = (1.0 - average_rate) * precision[core] + average_rate * square
        raw = grad / (fresh + damping)
        out[core, 2 * at] = raw
        out[core, 2 * at + 1] = fresh
        local = local + jnp.sum(raw * raw, axis=0, keepdims=True)
    folded = local[:, :128]
    for start in range(128, local.shape[1], 128):
        folded = folded + local[:, start : start + 128]
    parts[0] = jnp.broadcast_to(folded, (8, 128))
    pl.semaphore_wait(barrier, count)
    swap = pltpu.make_async_remote_copy(
        src_ref=out.at[core],
        dst_ref=out.at[core],
        send_sem=swap_send,
        recv_sem=swap_recv,
        device_id={"mc": 1 - core},
        device_id_type=pl.DeviceIdType.MESH,
    )
    slot = 0
    for stage, (name, size) in enumerate(axes):
        copies = []
        for shift in range(1, size):
            copy = pltpu.make_async_remote_copy(
                src_ref=parts.at[stage],
                dst_ref=got.at[slot + shift - 1],
                send_sem=part_send.at[slot + shift - 1],
                recv_sem=part_recv.at[slot + shift - 1],
                device_id={name: lax.rem(place[name] + shift, size)},
                device_id_type=pl.DeviceIdType.MESH,
            )
            copy.start()
            copies.append(copy)
        if stage == 0:
            swap.start()
        for copy in copies:
            copy.wait()
        value = parts[stage]
        for shift in range(1, size):
            value = value + got[slot + shift - 1]
        parts[stage + 1] = value
        slot += size - 1
    total[...] = parts[len(axes)]
    swap.wait()


def finish(sums_up, sums_down, precision_up, precision_down, images_all):
    axes = tuple((name, lax.axis_size(name)) for name in ("mc", "mp", "dp"))
    partners = sum(size - 1 for _, size in axes)
    half, width = sums_up.shape[1:]
    vmem = pl.BlockSpec(memory_space=pltpu.VMEM)
    return pl.pallas_call(
        functools.partial(finish_kernel, axes, images_all),
        out_shape=(
            jax.ShapeDtypeStruct((2, 4, half, width), jnp.float32),
            jax.ShapeDtypeStruct((8, 128), jnp.float32),
        ),
        in_specs=[vmem] * 4,
        out_specs=(vmem, vmem),
        scratch_shapes=[
            pltpu.VMEM((len(axes) + 1, 8, 128), jnp.float32),
            pltpu.VMEM((partners, 8, 128), jnp.float32),
            pltpu.SemaphoreType.DMA,
            pltpu.SemaphoreType.DMA,
            pltpu.SemaphoreType.DMA((partners,)),
            pltpu.SemaphoreType.DMA((partners,)),
        ],
        compiler_params=pltpu.CompilerParams(collective_id=0, has_side_effects=True),
        name="finish",
    )(
        sums_up,
        sums_down,
        precision_up.reshape(2, half, width),
        precision_down.reshape(2, half, width),
    )


def shards(
    features, out_cotangent, mean_up, precision_up, noise_up, mean_down, precision_down, noise_down
):
    shard_up = sample_weights(mean_up, precision_up, noise_up[0])
    shard_down = sample_weights(mean_down, precision_down, noise_down[0])
    w_up = lax.all_gather(shard_up, "dp", axis=0, tiled=True)
    w_down = lax.all_gather(shard_down, "dp", axis=0, tiled=True)
    cotangent = out_cotangent[0]
    preact = jnp.dot(features, w_up, preferred_element_type=jnp.float32)
    gelu_value, gelu_slope = gelu_parts(preact)
    hidden = gelu_value.astype(jnp.bfloat16)
    sums_down = reduce_images(*image_sums(cotangent, hidden))
    hidden_grad = jnp.dot(cotangent, w_down, preferred_element_type=jnp.float32)
    preact_grad = (hidden_grad * gelu_slope).astype(jnp.bfloat16)
    sums_up = reduce_images(*image_sums(features, preact_grad))
    input_grad = scatter_sum(contract_cols(preact_grad, w_up)).astype(jnp.bfloat16)[None]

    images_all = (features.shape[0] // PATCHES) * lax.axis_size("dp")
    halves, total = finish(sums_up, sums_down, precision_up, precision_down, images_all)
    raw_up, new_up, raw_down, new_down = [halves[:, at].reshape(mean_up.shape) for at in range(4)]
    root_mean = jnp.sqrt(jnp.sum(total[0]) / (2 * D * FF))
    factor = 1.0 / jnp.maximum(clip_level, root_mean)
    mean_new_up = mean_up - step_rate * factor * raw_up
    mean_new_down = mean_down - step_rate * factor * raw_down
    return (mean_new_up, new_up, mean_new_down, new_down, input_grad)


def solution(mesh):
    in_specs = (
        P("dp", None),
        P("mc", "dp", None),
        P("dp", "mp"),
        P("dp", "mp"),
        P("mc", "dp", "mp"),
        P("dp", "mp"),
        P("dp", "mp"),
        P("mc", "dp", "mp"),
    )
    out_specs = (P("dp", "mp"), P("dp", "mp"), P("dp", "mp"), P("dp", "mp"), P("mc", "dp", "mp"))
    return jax.shard_map(shards, mesh=mesh, in_specs=in_specs, out_specs=out_specs, check_vma=False)
```
